32 devices in a mesh: dp: 4 (over y, core), vocab: 8 (over z, x).
Axes of the slice: x: 2, y: 2, z: 4, core: 2. Of those that a mesh axis runs over, the one named last changes fastest.
Arguments:
- teacher_hidden: bfloat16 [512, 16384], P('dp', 'vocab'), may hold values from -120 to 120
- student_hidden: bfloat16 [512, 4096], P('dp', 'vocab'), may hold values from -120 to 120
- teacher_weight: bfloat16 [16384, 65536], P('dp', 'vocab'), may hold values from -1 to 1
- student_weight: bfloat16 [4096, 65536], P('dp', 'vocab'), may hold values from -1 to 1
Outputs:
- kl: float32 [512], P('dp')
- loss: float32 [], replicated
The draws below stay inside these ranges and needn't reach their ends.
All inputs are finite; a program needn't handle non-finite values.
Results may differ from the reference program's by a relative error of at most 0.0003.
Values may be sent and summed in bfloat16 or wider, within the bound.
No kernel may reach another device: no remote copies, remote signals or barrier semaphores. Data moves between devices by JAX's collectives and lax.ppermute only.
A program may use at most 256 MiB of HBM per device.

```python
import jax
import jax.numpy as jnp

HT = 16384
HS = 4096
V = 65536
TOKENS = 512


def weight_block(key, offset, features, block_id):
    normals = jax.random.normal(jax.random.fold_in(jax.random.fold_in(key, offset), block_id), (features, 128), jnp.float32)
    return jnp.clip(normals, -6.0, 6.0) * features ** (-0.5)


def teacher_block(key, block_id):
    return weight_block(key, 101, HT, block_id)


def student_block(key, block_id):
    folded = teacher_block(key, block_id).reshape(HT // HS, HS, 128).sum(axis=0)
    own_noise = weight_block(key, 202, HS, block_id)
    return jnp.clip(folded + 0.1 * own_noise, -1.0, 1.0)


def stack_blocks(key, block_fn, features):
    tile_stack = jax.vmap(lambda block_id: block_fn(key, block_id))(jnp.arange(V // 128))
    return jnp.transpose(tile_stack, (1, 0, 2)).reshape(features, V)


def shared_rows(key):
    common = jax.random.normal(jax.random.fold_in(key, 11), (TOKENS, HS), jnp.float32) * 3.0
    rising = 1.0 + 0.85 * jnp.arange(TOKENS, dtype=jnp.float32) / TOKENS
    return (common, rising)


def draw_teacher_weight(key, part):
    return stack_blocks(key, teacher_block, HT).astype(jnp.bfloat16)


def draw_student_weight(key, part):
    return stack_blocks(key, student_block, HS).astype(jnp.bfloat16)


def draw_teacher_hidden(key, part):
    common, rising = shared_rows(key)
    own_noise = jax.random.normal(jax.random.fold_in(key, 12), (TOKENS, HT), jnp.float32) * 0.5 * rising[:, None]
    values = jnp.tile(common, (1, HT // HS)) + own_noise
    return jnp.clip(values, -120.0, 120.0).astype(jnp.bfloat16)


def draw_student_hidden(key, part):
    common, rising = shared_rows(key)
    own_noise = jax.random.normal(jax.random.fold_in(key, 32), (TOKENS, HS), jnp.float32) * 0.5 * rising[:, None]
    values = common + own_noise
    return jnp.clip(values, -120.0, 120.0).astype(jnp.bfloat16)


def setup_inputs(seed: int = 0) -> dict:
    keys = jax.random.split(jax.random.key(seed), 5)
    teacher_hidden = draw_teacher_hidden(jax.random.fold_in(keys[4], 71), 0)
    student_hidden = draw_student_hidden(jax.random.fold_in(keys[4], 71), 0)
    teacher_weight = draw_teacher_weight(jax.random.fold_in(keys[4], 71), 0)
    student_weight = draw_student_weight(jax.random.fold_in(keys[4], 71), 0)
    return dict(teacher_hidden=teacher_hidden, student_hidden=student_hidden, teacher_weight=teacher_weight, student_weight=student_weight)


def reference(teacher_hidden, student_hidden, teacher_weight, student_weight):
    teacher_logits = jnp.dot(teacher_hidden, teacher_weight, preferred_element_type=jnp.float32)
    student_logits = jnp.dot(student_hidden, student_weight, preferred_element_type=jnp.float32)
    teacher_top = jnp.max(teacher_logits, axis=1)
    student_top = jnp.max(student_logits, axis=1)
    teacher_exp = jnp.exp(teacher_logits - teacher_top[:, None])
    teacher_total = jnp.sum(teacher_exp, axis=1)
    weighted = jnp.sum(teacher_exp * (teacher_logits - student_logits), axis=1)
    student_total = jnp.sum(jnp.exp(student_logits - student_top[:, None]), axis=1)
    teacher_lse = teacher_top + jnp.log(teacher_total)
    student_lse = student_top + jnp.log(student_total)
    kl = weighted / teacher_total - teacher_lse + student_lse
    loss = jnp.mean(kl)
    return (kl, loss)
```

```python
import functools
import math

import jax
import jax.numpy as jnp
from jax import lax
from jax.experimental import pallas as pl
from jax.experimental.pallas import tpu as pltpu
from jax.sharding import PartitionSpec as P


LANES = 128
F32 = jnp.float32
BF16 = jnp.bfloat16
SPAN, OFFSET = 248.0, 124.0
CHUNKS = {"S": (3, 5), "T": (3, 2, 2, 1)}
FIRST = (5, 3)


def block_of(n, most):
    while n % most:
        most //= 2
    return most


def assemble_kernel(where_ref, *refs, first, parts):
    *hidden, rows_ref = refs
    tok, feat = hidden[0].shape
    for i, piece in enumerate(hidden):
        row = pl.multiple_of(where_ref[2 * (first + i) + 1] * tok, tok)
        part = where_ref[2 * (first + i)]
        if parts * feat > rows_ref.shape[1]:
            part = part // 2
        for p in range(rows_ref.shape[1] // feat):

            @pl.when(part == p)
            def _(piece=piece, p=p, row=row):
                rows_ref[pl.ds(row, tok), p * feat : (p + 1) * feat] = piece[...]


def assemble(where, hidden, first, slots, parts):
    tok, feat = hidden[0].shape
    return pl.pallas_call(
        functools.partial(assemble_kernel, first=first, parts=parts),
        in_specs=[pl.BlockSpec(memory_space=pltpu.SMEM)]
        + [pl.BlockSpec(memory_space=pltpu.VMEM)] * len(hidden),
        out_specs=pl.BlockSpec(memory_space=pltpu.VMEM),
        out_shape=jax.ShapeDtypeStruct((slots * tok, len(hidden) * feat // slots), BF16),
        compiler_params=pltpu.CompilerParams(vmem_limit_bytes=12 * 2**20),
    )(where, *hidden)


def spans(width, shares):
    edges = [width * sum(shares[:i]) // sum(shares) for i in range(len(shares) + 1)]
    return [(a, b - a) for a, b in zip(edges, edges[1:])]


def holder(chunks, start):
    return max(i for i, (first, _) in enumerate(chunks) if first <= start)


def matmul_kernel(which_ref, rows_ref, *refs, count, base, split):
    weights = refs[:count]
    outs = refs[count + base :]
    feat = weights[0].shape[0]
    total = refs[count][...] if base else None
    for i, weight in enumerate(weights):
        dot = jnp.dot(
            rows_ref[:, i * feat : (i + 1) * feat], weight[...], preferred_element_type=F32
        )
        total = dot if total is None else total + dot
    if split:
        half = total.shape[0] // 2
        outs[0][...] = total[:half]
        outs[1][...] = total[half:]
    else:
        outs[0][...] = total


def matmul(which, rows, weight, start, width, bn, parts=1, base=None, split=True):
    count, depth = rows.shape
    bn = block_of(math.gcd(width, start, base[1] if base else 0), bn)
    blocks = max(parts // 2, 1)
    feat = depth // blocks
    specs = [pl.BlockSpec((count, depth), lambda j, w: (0, 0))]
    for i in range(blocks):
        specs.append(
            pl.BlockSpec(
                (feat, bn),
                lambda j, w, i=i: ((2 * i + w[0]) if parts > 1 else 0, start // bn + j),
            )
        )
    args = [rows] + [weight] * blocks
    if base is not None:
        specs.append(pl.BlockSpec((count, bn), lambda j, w: (0, base[1] // bn + j)))
        args.append(base[0])
    outs = 2 if split else 1
    return pl.pallas_call(
        functools.partial(
            matmul_kernel, count=blocks, base=int(base is not None), split=split
        ),
        grid_spec=pltpu.PrefetchScalarGridSpec(
            num_scalar_prefetch=1,
            grid=(width // bn,),
            in_specs=specs,
            out_specs=[pl.BlockSpec((count // outs, bn), lambda j, w: (0, j))] * outs,
        ),
        out_shape=[jax.ShapeDtypeStruct((count // outs, width), F32)] * outs,
        compiler_params=pltpu.CompilerParams(
            dimension_semantics=("arbitrary",), vmem_limit_bytes=24 * 2**20
        ),
        cost_estimate=pl.CostEstimate(
            flops=2 * count * depth * width,
            bytes_accessed=2 * depth * width + 4 * count * width,
            transcendentals=0,
        ),
    )(which, *args)


def encode_kernel(keep_ref, recv_ref, code_ref, own_ref):
    rows, width = code_ref.shape[0], keep_ref.shape[1]
    value = keep_ref[:rows] + recv_ref[:rows]
    size = jnp.abs(value)
    top = jnp.max(size, axis=1, keepdims=True)
    scale = jnp.maximum(top * 1.01, 1e-30).astype(BF16)
    power = jnp.exp2(size * (SPAN / scale.astype(F32)) - OFFSET)
    code_ref[:, :width] = jnp.where(value < 0.0, -power, power).astype(BF16)
    code_ref[:, width:] = jnp.broadcast_to(scale, (rows, LANES))
    own_ref[...] = keep_ref[rows:] + recv_ref[rows:]


def encode(keep, recv, tok, bn):
    total, width = keep.shape
    rows = total - tok
    steps = width // bn
    return pl.pallas_call(
        encode_kernel,
        grid=(steps,),
        in_specs=[pl.BlockSpec((total, bn), lambda j: (0, j))] * 2,
        out_specs=[
            pl.BlockSpec((rows, bn + LANES), lambda j: (0, j)),
            pl.BlockSpec((tok, bn), lambda j: (0, j)),
        ],
        out_shape=[
            jax.ShapeDtypeStruct((rows, steps * (bn + LANES)), BF16),
            jax.ShapeDtypeStruct((tok, width), F32),
        ],
        compiler_params=pltpu.CompilerParams(
            dimension_semantics=("arbitrary",), vmem_limit_bytes=24 * 2**20
        ),
        cost_estimate=pl.CostEstimate(
            flops=8 * total * width,
            bytes_accessed=12 * total * width,
            transcendentals=rows * width,
        ),
    )(keep, recv)


def decoded(code, scale):
    power = code.astype(F32)
    size = (jnp.log2(jnp.abs(power)) + OFFSET) * (scale.astype(F32) * (1.0 / SPAN))
    return jnp.where(power < 0.0, -size, size)


def own_logits(own_ref, codes):
    total = own_ref[...]
    bn = total.shape[1]
    for code in codes:
        width = code.shape[1] - LANES
        column = pl.multiple_of(pl.program_id(0) * bn % width, LANES)
        total += decoded(code[:, pl.ds(column, bn)], code[:, width : width + 1])
    return total


def columns_of(old, columns):
    lane = lax.broadcasted_iota(jnp.int32, old.shape, 1)
    new = old
    for i, column in columns.items():
        new = jnp.where(lane == i, column, new)
    return new


def student_kernel(own_ref, *refs, others):
    codes = refs[:others]
    prev_ref, logit_ref, out_ref = refs[others:]

    @pl.when(pl.program_id(0) == 0)
    def _():
        out_ref[...] = prev_ref[...]

    s = own_logits(own_ref, codes)
    logit_ref[...] = s
    old = out_ref[...]
    top = jnp.maximum(old[:, 3:4], jnp.max(s, axis=1, keepdims=True))
    total = old[:, 4:5] * jnp.exp(old[:, 3:4] - top) + jnp.sum(
        jnp.exp(s - top), axis=1, keepdims=True
    )
    out_ref[...] = columns_of(old, {3: top, 4: total})


def teacher_kernel(own_ref, *refs, others, last):
    codes = refs[:others]
    logit_ref, prev_ref, out_ref, acc_ref = refs[others:]
    step = pl.program_id(0)

    @pl.when(step == 0)
    def _():
        acc_ref[...] = prev_ref[...]

    t = own_logits(own_ref, codes)
    old = acc_ref[...]
    top = jnp.maximum(old[:, 0:1], jnp.max(t, axis=1, keepdims=True))
    size = jnp.exp(t - top)
    fade = jnp.exp(old[:, 0:1] - top)
    total = old[:, 1:2] * fade + jnp.sum(size, axis=1, keepdims=True)
    weighted = old[:, 2:3] * fade + jnp.sum(size * (t - logit_ref[...]), axis=1, keepdims=True)
    new = columns_of(old, {0: top, 1: total, 2: weighted})
    acc_ref[...] = new

    @pl.when(step == pl.num_programs(0) - 1)
    def _():
        if last:
            out_ref[...] = jnp.transpose(new)[:8]
        else:
            out_ref[...] = new


def stats(chunk, tok, prev, logit=None, start=0, last=False):
    own, codes, code_block = chunk
    width = own.shape[1]
    bn = block_of(math.gcd(code_block, start), 1024)
    per = code_block // bn
    whole = pl.BlockSpec((tok, LANES), lambda j: (0, 0))
    specs = [pl.BlockSpec((tok, bn), lambda j: (0, j))]
    specs += [pl.BlockSpec((tok, code_block + LANES), lambda j: (0, j // per))] * len(codes)
    args = [own, *codes]
    scratch = []
    if logit is None:
        kernel = functools.partial(student_kernel, others=len(codes))
        out_specs = [pl.BlockSpec((tok, bn), lambda j: (0, j)), whole]
        out_shape = [
            jax.ShapeDtypeStruct((tok, width), F32),
            jax.ShapeDtypeStruct((tok, LANES), F32),
        ]
    else:
        kernel = functools.partial(teacher_kernel, others=len(codes), last=last)
        specs.append(pl.BlockSpec((tok, bn), lambda j: (0, start // bn + j)))
        args.append(logit)
        shape = (8, tok) if last else (tok, LANES)
        out_specs = pl.BlockSpec(shape, lambda j: (0, 0))
        out_shape = jax.ShapeDtypeStruct(shape, F32)
        scratch = [pltpu.VMEM((tok, LANES), F32)]
    return pl.pallas_call(
        kernel,
        grid=(width // bn,),
        in_specs=specs + [whole],
        out_specs=out_specs,
        out_shape=out_shape,
        scratch_shapes=scratch,
        compiler_params=pltpu.CompilerParams(
            dimension_semantics=("arbitrary",), vmem_limit_bytes=14 * 2**20
        ),
        cost_estimate=pl.CostEstimate(
            flops=20 * tok * width, bytes_accessed=14 * tok * width, transcendentals=2 * tok * width
        ),
    )(*args, prev)


def merge(a, b):
    t_top, s_top = jnp.maximum(a[0:1], b[0:1]), jnp.maximum(a[3:4], b[3:4])
    ta, tb = jnp.exp(a[0:1] - t_top), jnp.exp(b[0:1] - t_top)
    sa, sb = jnp.exp(a[3:4] - s_top), jnp.exp(b[3:4] - s_top)
    return jnp.concatenate(
        [t_top, a[1:3] * ta + b[1:3] * tb, s_top, a[4:5] * sa + b[4:5] * sb, a[5:8]], axis=0
    )


def shards(teacher_hidden, student_hidden, teacher_weight, student_weight):
    nd, nv = lax.axis_size("dp"), lax.axis_size("vocab")
    chips = nd // 2
    r = nv // nd
    ring = nv // 2
    tok = teacher_hidden.shape[0]
    vocab = teacher_weight.shape[1]
    d, v = lax.axis_index("dp"), lax.axis_index("vocab")

    def place(group):
        return (group % 2) * chips + group // 2

    shuffle = [
        (g * nv + f, (f // r) * nv + place(g) * r + f % r) for g in range(nd) for f in range(nv)
    ]
    turn = [(i, (i + 2) % nv) for i in range(nv)]
    flip = [(i, i ^ 1) for i in range(nv)]

    where = []
    for b in range(2):
        for k in range(ring):
            j = ((v // 2 - k) % ring) * 2 + (v % 2) ^ b
            group, part = j // r, j % r
            core, chip = group // chips, group % chips
            ahead = (chip - d // 2 - 1) % chips
            slot = jnp.where(core == d % 2, chips, 0) + ahead
            where += [part, slot]
    where = jnp.stack(where).astype(jnp.int32)

    parity = jnp.reshape(v % 2, (1,)).astype(jnp.int32)
    partner = [(i, i ^ 1) for i in range(nd)]

    def across(code):
        codes = []
        for o in range(1, chips):
            to = [(y * 2 + c, ((y + o) % chips) * 2 + c) for y in range(chips) for c in range(2)]
            codes.append(lax.ppermute(code[(o - 1) * tok : o * tok], "dp", to))
        return codes

    def gather(hidden):
        pieces = [lax.ppermute(hidden, ("dp", "vocab"), shuffle)]
        flips = []
        for k in range(ring):
            flips.append(lax.ppermute(pieces[k], "vocab", flip))
            if k < ring - 1:
                pieces.append(lax.ppermute(pieces[k], "vocab", turn))
        return pieces, flips

    def exchange(send, keep):
        width = keep.shape[1]
        steps = -(-width // 3072)
        while width % (steps * LANES):
            steps += 1
        code_block = width // steps
        recv = lax.ppermute(send, "dp", partner)
        code, own = encode(keep, recv, tok, code_block)
        return own, across(code), code_block

    student, teacher = [], []
    turns, flips = gather(student_hidden)
    student_weight = pltpu.with_memory_space_constraint(student_weight, pltpu.HBM)
    rows = assemble(where, turns + flips, 0, nd, r)
    s_spans = spans(vocab, CHUNKS["S"])
    for start, width in s_spans:
        send, keep = matmul(parity, rows, student_weight, start, width, 1024)
        student.append(exchange(send, keep))

    turns, flips = gather(teacher_hidden)
    rows = assemble(where, turns, 0, nd, r)
    bases = []
    b_spans = spans(vocab, FIRST)
    for start, width in b_spans:
        bases += matmul(parity, rows, teacher_weight, start, width, 512, parts=r, split=False)
    rows = assemble(where, flips, ring, nd, r)
    t_spans = spans(vocab, CHUNKS["T"])
    for start, width in t_spans:
        k = holder(b_spans, start)
        base = (bases[k], start - b_spans[k][0])
        send, keep = matmul(1 - parity, rows, teacher_weight, start, width, 512, parts=r, base=base)
        teacher.append(exchange(send, keep))

    lane = lax.broadcasted_iota(jnp.int32, (tok, LANES), 1)
    run = jnp.where((lane == 0) | (lane == 3), -3.0e38, 0.0).astype(F32)
    logits = []
    for chunk in student:
        logit, run = stats(chunk, tok, run)
        logits.append(logit)
    for i, chunk in enumerate(teacher):
        k = holder(s_spans, t_spans[i][0])
        start = t_spans[i][0] - s_spans[k][0]
        run = stats(chunk, tok, run, logits[k], start, i == len(teacher) - 1)

    bit = 1
    while bit < nv:
        run = merge(run, lax.ppermute(run, "vocab", [(i, i ^ bit) for i in range(nv)]))
        bit *= 2
    kl = run[2] / run[1] - (run[0] + jnp.log(run[1])) + (run[3] + jnp.log(run[4]))
    loss = lax.psum(jnp.sum(kl), "dp") / (tok * nd)
    return (kl, loss)


def solution(mesh):
    spec = P("dp", "vocab")

    return jax.shard_map(
        shards, mesh=mesh, in_specs=(spec,) * 4, out_specs=(P("dp"), P()), check_vma=False
    )
```
